32 devices in a mesh: gx: 2 (over x), gy: 4 (over y, core), gz: 4 (over z).
Axes of the slice: x: 2, y: 2, z: 4, core: 2. Of those that a mesh axis runs over, the one named last changes fastest.
Arguments:
- ambient_motion_array: float32 [3, 16, 256, 512], P(None, 'gx', 'gy', 'gz'), may hold values from -6 to 6
- ambient_scalar_trio: float32 [3, 16, 256, 512], P(None, 'gx', 'gy', 'gz'), may hold values from 0.2 to 1
- droplet_local_position: float32 [3, 32768], P(None, ('gx', 'gy', 'gz')), may hold values from -0.5 to 0.5
- droplet_motion_array: float32 [3, 32768], P(None, ('gx', 'gy', 'gz')), may hold values from -6 to 6
- droplet_heat_level: float32 [32768], P(('gx', 'gy', 'gz')), may hold values from 0.3 to 0.9
- droplet_size_quadratic: float32 [32768], P(('gx', 'gy', 'gz')), may hold values from 0.25 to 4
- local_i_position: int32 [32768], P(('gx', 'gy', 'gz')), may hold values from 0 to 7
- local_j_position: int32 [32768], P(('gx', 'gy', 'gz')), may hold values from 0 to 63
- local_k_position: int32 [32768], P(('gx', 'gy', 'gz')), may hold values from 0 to 127
- active_group_tally: int32 [32], P(('gx', 'gy', 'gz')), may hold values from 1 to 8, as said below
Outputs:
- gas_source: float32 [5, 16, 256, 512], P(None, 'gx', 'gy', 'gz')
- parcel_state: float32 [5, 32768], P(None, ('gx', 'gy', 'gz'))
The draws below stay inside these ranges and needn't reach their ends.
Inputs may be any that keep to these rules, and one draw needn't show every extreme that they name: `active_group_tally`: tiles of a brick are live from the first one on; in every draw some brick has all 8 tiles live.
All inputs are finite; a program needn't handle non-finite values.
Results may differ from the reference program's by a relative error of at most 0.0003.
Values sent between devices are 32-bit elements; how exact they have to be, the bound alone decides.
A program may use at most 128 MiB of HBM per device.

```python
import math
import jax
import jax.numpy as jnp
from jax import lax

CX = 8
CY = 64
CZ = 128
TILE = 128
TILE_CAP = 8
PAR_DEV = 1024
BRICKS = 32
GRID_EXTENT_I = 16
GRID_EXTENT_J = 256
GRID_EXTENT_K = 512
SPRAY_CAPACITY_N = 32768
N_GY = 4
N_GZ = 4


def draw_active_group_tally(key, part):
    key_base, key_core, key_pick = jax.random.split(key, 3)
    lowest = max(1, TILE_CAP // 4)
    highest = max(lowest + 1, TILE_CAP // 2 + 1)
    base_tiles = jax.random.randint(key_base, (BRICKS,), lowest, highest)
    dense_brick = jax.random.randint(key_core, (BRICKS,), 0, 8) == 0
    chosen = jax.random.randint(key_pick, (), 0, BRICKS)
    dense_brick = dense_brick | (jnp.arange(BRICKS) == chosen)
    return jnp.where(dense_brick, TILE_CAP, base_tiles).astype(jnp.int32)


def plant(array, stream_key, low, top_value):
    dims = array.shape
    spot = [jax.random.randint(jax.random.fold_in(stream_key, axis), (), 0, dims[axis]) for axis in range(len(dims))]
    array = array.at[tuple(spot)].set(low)
    longest = dims.index(max(dims))
    spot[longest] = (spot[longest] + 1) % dims[longest]
    return array.at[tuple(spot)].set(top_value)


def block_scale(stream_key, shape, cuts, smallest, top_value):
    gain = 1.0
    for position, parts in cuts:
        heights = jax.random.uniform(jax.random.fold_in(jax.random.fold_in(stream_key, 6), position), (parts,), jnp.float32, smallest / len(cuts), top_value / len(cuts))
        gain = gain * jnp.repeat(jnp.exp(heights), shape[position] // parts).reshape((-1,) + (1,) * (len(shape) - 1 - position))
    return gain


def normal_values(stream_key, dims, deviation, limit, pieces=(), held_as=jnp.bfloat16):
    entries = jax.random.normal(stream_key, dims, jnp.float32) * deviation
    if len(pieces) > 0:
        entries = block_scale(stream_key, dims, pieces, -0.22, 0.18) * entries
    return jnp.clip(entries, min=-limit, max=limit).astype(held_as)


def setup_inputs(seed: int = 0) -> dict:
    key_of = jax.random.split(jax.random.key(seed), 11)
    ambient_motion_array = normal_values(key_of[0], (3, GRID_EXTENT_I, GRID_EXTENT_J, GRID_EXTENT_K), 1.0, 6.0, ((1, 2), (2, 4), (3, 4)), jnp.float32)
    ambient_scalar_trio = jnp.clip(0.2 + 0.8 * jax.random.uniform(key_of[1], (3, GRID_EXTENT_I, GRID_EXTENT_J, GRID_EXTENT_K), jnp.float32) ** block_scale(key_of[1], (3, GRID_EXTENT_I, GRID_EXTENT_J, GRID_EXTENT_K), ((1, 2), (2, 4), (3, 4)), -0.2, 0.2), 0.2, 1.0)
    droplet_local_position = jnp.clip(jax.random.uniform(key_of[2], (3, SPRAY_CAPACITY_N), jnp.float32, -0.5, 0.5) * block_scale(key_of[2], (3, SPRAY_CAPACITY_N), ((1, 32),), -0.4, 0.0), -0.5, 0.5)
    droplet_motion_array = normal_values(key_of[3], (3, SPRAY_CAPACITY_N), 1.0, 6.0, ((1, 32),), jnp.float32)
    droplet_heat_level = jnp.clip(0.3 + 0.59999996 * jax.random.uniform(key_of[4], (SPRAY_CAPACITY_N,), jnp.float32) ** block_scale(key_of[4], (SPRAY_CAPACITY_N,), ((0, 32),), -0.2, 0.2), 0.3, 0.9)
    droplet_size_quadratic = jnp.clip(jnp.exp(math.log(4.0) - 2.7725887 * jax.random.uniform(key_of[5], (SPRAY_CAPACITY_N,), jnp.float32) ** block_scale(key_of[5], (SPRAY_CAPACITY_N,), ((0, 32),), -0.2, 0.2)), 0.25, 4.0)
    local_i_position = plant(jax.random.randint(key_of[6], (SPRAY_CAPACITY_N,), 0, CX), jax.random.fold_in(key_of[6], 1), 0, CX - 1).astype(jnp.int32)
    local_j_position = plant(jax.random.randint(key_of[7], (SPRAY_CAPACITY_N,), 0, CY), jax.random.fold_in(key_of[7], 1), 0, CY - 1).astype(jnp.int32)
    local_k_position = plant(jax.random.randint(key_of[8], (SPRAY_CAPACITY_N,), 0, CZ), jax.random.fold_in(key_of[8], 1), 0, CZ - 1).astype(jnp.int32)
    active_group_tally = draw_active_group_tally(jax.random.fold_in(key_of[10], 71), 0)
    return {"ambient_motion_array": ambient_motion_array, "ambient_scalar_trio": ambient_scalar_trio, "droplet_local_position": droplet_local_position, "droplet_motion_array": droplet_motion_array, "droplet_heat_level": droplet_heat_level, "droplet_size_quadratic": droplet_size_quadratic, "local_i_position": local_i_position, "local_j_position": local_j_position, "local_k_position": local_k_position, "active_group_tally": active_group_tally}


step_time = 0.25
evap_rate = 1.0
heat_rate = 2.0
boiling_energy_drain = 0.3

def tent_weights(offset_values):
    shifts = jnp.arange(3, dtype=jnp.float32) - 1.0
    return jnp.maximum(0.0, 1.0 - jnp.abs(offset_values[:, None, :] - shifts[None, :, None]))

def integrate_droplets(sampled_ambient_quantities, sampled_motion, sampled_heat_level, diam_quadratic_entry):
    ambient_motion = sampled_ambient_quantities[0:3]
    ambient_heat_level = sampled_ambient_quantities[3]
    ambient_moisture = sampled_ambient_quantities[4]
    ambient_rho_level = sampled_ambient_quantities[5]
    drag_ratio = step_time / (0.5 * diam_quadratic_entry)
    revised_speed = (sampled_motion + drag_ratio * ambient_motion) / (1.0 + drag_ratio)
    blob_weight_kilos = diam_quadratic_entry * jnp.sqrt(diam_quadratic_entry)
    vapour_equilibrium_share = jnp.exp(4.0 * (sampled_heat_level - 1.0))
    decay_multiplier = step_time * evap_rate * ambient_rho_level * (vapour_equilibrium_share - ambient_moisture)
    next_width_power = diam_quadratic_entry - decay_multiplier
    revised_weight = next_width_power * jnp.sqrt(next_width_power)
    conduction_intensity = step_time * heat_rate * ambient_rho_level / diam_quadratic_entry
    fresh_heat_level = (sampled_heat_level + conduction_intensity * ambient_heat_level) / (1.0 + conduction_intensity) - boiling_energy_drain * decay_multiplier / diam_quadratic_entry
    momentum_energy_deposits = jnp.concatenate([blob_weight_kilos[None] * (sampled_motion - revised_speed), (blob_weight_kilos * (sampled_heat_level - fresh_heat_level))[None], (blob_weight_kilos - revised_weight)[None]], axis=0)
    fresh_droplet_entry = jnp.concatenate([revised_speed, fresh_heat_level[None], next_width_power[None]], axis=0)
    return (fresh_droplet_entry, momentum_energy_deposits)

def reference(ambient_motion_array, ambient_scalar_trio, droplet_local_position, droplet_motion_array, droplet_heat_level, droplet_size_quadratic, local_i_position, local_j_position, local_k_position, active_group_tally):
    maximum_droplets_held = droplet_heat_level.shape[0]
    slot_id = jnp.arange(maximum_droplets_held, dtype=jnp.int32)
    brick_id = slot_id // PAR_DEV
    live_slot = slot_id % PAR_DEV // TILE < active_group_tally[brick_id]
    glob_x = brick_id // (N_GY * N_GZ) * CX + local_i_position
    glob_y = brick_id // N_GZ % N_GY * CY + local_j_position
    glob_z = brick_id % N_GZ * CZ + local_k_position
    quantity_bundle = jnp.concatenate([ambient_motion_array, ambient_scalar_trio], axis=0).reshape(6, -1)
    tent_table = tent_weights(droplet_local_position)
    vertex_weightings = jnp.arange(27, dtype=jnp.int32)
    cell_total = GRID_EXTENT_I * GRID_EXTENT_J * GRID_EXTENT_K

    def locate(stencil):
        pos_x = glob_x + stencil // 9 - 1
        pos_y = glob_y + stencil // 3 % 3 - 1
        pos_z = glob_z + stencil % 3 - 1
        inside = (pos_x >= 0) & (pos_x < GRID_EXTENT_I) & (pos_y >= 0) & (pos_y < GRID_EXTENT_J) & (pos_z >= 0) & (pos_z < GRID_EXTENT_K)
        flat_idx = (jnp.clip(pos_x, 0, GRID_EXTENT_I - 1) * GRID_EXTENT_J + jnp.clip(pos_y, 0, GRID_EXTENT_J - 1)) * GRID_EXTENT_K + jnp.clip(pos_z, 0, GRID_EXTENT_K - 1)
        weight = tent_table[0, stencil // 9] * tent_table[1, stencil // 3 % 3] * tent_table[2, stencil % 3]
        weight = jnp.where(inside, weight, 0.0)
        return (flat_idx.astype(jnp.int32), weight, inside)

    def sample_routine(running, stencil):
        flat_idx, weight, inside = locate(stencil)
        return (running + weight[None] * quantity_bundle[:, flat_idx], None)
    sampled_ambient_quantities = lax.scan(sample_routine, jnp.zeros((6, maximum_droplets_held), jnp.float32), vertex_weightings)[0]
    fresh_droplet_entry, momentum_energy_deposits = integrate_droplets(sampled_ambient_quantities, droplet_motion_array, droplet_heat_level, droplet_size_quadratic)
    momentum_energy_deposits = jnp.where(live_slot[None], momentum_energy_deposits, 0.0)

    def deposit_step(running, stencil):
        flat_idx, weight, inside = locate(stencil)
        target = jnp.where(inside, flat_idx, cell_total).astype(jnp.int32)
        return (running.at[:, target].add(weight[None] * momentum_energy_deposits, mode='drop'), None)
    deposit = lax.scan(deposit_step, jnp.zeros((5, cell_total), jnp.float32), vertex_weightings)[0]
    forwarded_carry = jnp.concatenate([droplet_motion_array, droplet_heat_level[None], droplet_size_quadratic[None]], axis=0)
    parcel_state = jnp.where(live_slot[None], fresh_droplet_entry, forwarded_carry)
    return (deposit.reshape(5, GRID_EXTENT_I, GRID_EXTENT_J, GRID_EXTENT_K), parcel_state)
```

```python
import functools

import jax
import jax.numpy as jnp
from jax import lax
from jax.experimental import pallas as pl
from jax.experimental.pallas import tpu as pltpu
from jax.sharding import PartitionSpec as P

TILE = 128
AXES = ("gx", "gy", "gz")
MESH = pl.DeviceIdType.MESH
F32 = jnp.float32
BF16 = jnp.bfloat16

step_time = 0.25
evap_rate = 1.0
heat_rate = 2.0
boiling_energy_drain = 0.3

X_MOVES = ((1, 0, 0, 0), (-1, 0, 0, 1))
Y_MOVES = ((0, 1, 0, 0), (0, -1, 0, 1))
XY_MOVES = ((1, 1, 0, 0), (1, -1, 0, 1), (-1, 1, 0, 2), (-1, -1, 0, 3))
Z_MOVES = ((0, 0, 1, 0), (0, 0, -1, 1))


def split(value):
    high = value.astype(BF16)
    return high, (value - high.astype(F32)).astype(BF16)


def nn(a, b):
    return lax.dot_general(a, b, (((1,), (0,)), ((), ())), preferred_element_type=F32)


def nt(a, b):
    return lax.dot_general(a, b, (((1,), (1,)), ((), ())), preferred_element_type=F32)


def tn(a, b):
    return lax.dot_general(a, b, (((0,), (0,)), ((), ())), preferred_element_type=F32)


def pair_weights(offset):
    lower = jnp.where(offset < 0.0, -1.0, 0.0)
    first = jnp.maximum(0.0, 1.0 - jnp.abs(offset - lower))
    second = jnp.maximum(0.0, 1.0 - jnp.abs(offset - (lower + 1.0)))
    return first, second, jnp.where(offset < 0.0, -1, 0)


def kernel(
    counts,
    vel,
    sca,
    pos,
    mot,
    heat,
    size,
    li,
    lj,
    lk,
    tally,
    dep,
    state,
    fields,
    ft_hi,
    ft_lo,
    w_hi,
    w_lo,
    line,
    src_hi,
    src_lo,
    sampled,
    xh,
    yh,
    xyh,
    zh,
    ys,
    xys,
    zs,
    dxs,
    dys,
    dxys,
    dzs,
    dxr,
    dyr,
    dxyr,
    dzr,
    load_sem,
    send_sem,
    recv_sem,
):
    ci, cj, ck = vel.shape[1:]
    slots = heat.shape[1]
    inner = ci * cj
    planes = w_hi.shape[0]
    outer = planes - inner
    y_row = 2 * cj
    xy_row = y_row + 2 * ci
    me = [lax.axis_index(axis) for axis in AXES]

    def exists(move, sign):
        good = None
        for d in range(3):
            step = sign * move[d]
            if step == 1:
                test = me[d] < counts[d] - 1
            elif step == -1:
                test = me[d] > 0
            else:
                continue
            good = test if good is None else jnp.logical_and(good, test)
        return good

    def peer(move):
        return tuple(lax.rem(me[d] + move[d] + counts[d], counts[d]) for d in range(3))

    moves = X_MOVES + Y_MOVES + XY_MOVES + Z_MOVES

    class Message:
        def __init__(self, number, move, src, dst):
            self.move = move
            self.dst = dst
            self.copy = pltpu.make_async_remote_copy(
                src_ref=src,
                dst_ref=dst,
                send_sem=send_sem.at[number],
                recv_sem=recv_sem.at[number],
                device_id=peer(move),
                device_id_type=MESH,
            )

        def start(self):
            @pl.when(exists(self.move, 1))
            def _():
                self.copy.start()

        def blank(self):
            @pl.when(jnp.logical_not(exists(self.move, -1)))
            def _():
                self.dst[...] = jnp.zeros(self.dst.shape, F32)

        def arrive(self):
            @pl.when(exists(self.move, -1))
            def _():
                self.copy.wait_recv()

        def leave(self):
            @pl.when(exists(self.move, 1))
            def _():
                self.copy.wait_send()

    x_in, y_in, z_in, x_out, xy_out, z_out = [], [], [], [], [], []
    number = 0

    def add(group, move, src, dst):
        nonlocal number
        group.append(Message(number, move, src, dst))
        number += 1

    for move in X_MOVES:
        row = ci - 1 if move[0] > 0 else 0
        add(x_in, move, vel.at[:, row], xh.at[move[3], 0:3])
        add(x_in, move, sca.at[:, row], xh.at[move[3], 3:6])
    for move in Y_MOVES:
        add(y_in, move, ys.at[move[3]], yh.at[move[3]])
    for move in XY_MOVES:
        add(y_in, move, xys.at[move[3]], xyh.at[move[3]])
    for move in Z_MOVES:
        add(z_in, move, zs.at[move[3]], zh.at[move[3]])
    for move in Z_MOVES:
        add(z_out, move, dzs.at[move[3]], dzr.at[move[3]])
    for move in X_MOVES:
        add(x_out, move, dxs.at[move[3]], dxr.at[move[3]])
    for move in Y_MOVES:
        add(xy_out, move, dys.at[move[3]], dyr.at[move[3]])
    for move in XY_MOVES:
        add(xy_out, move, dxys.at[move[3]], dxyr.at[move[3]])

    barrier = pltpu.get_barrier_semaphore()
    for move in moves:

        @pl.when(exists(move, 1))
        def _():
            pl.semaphore_signal(barrier, inc=1, device_id=peer(move), device_id_type=MESH)

    loads = [
        pltpu.make_async_copy(vel, fields.at[0:3], load_sem.at[0]),
        pltpu.make_async_copy(sca, fields.at[3:6], load_sem.at[1]),
    ]
    for load in loads:
        load.start()
    for message in x_in + y_in + z_in + z_out + x_out + xy_out:
        message.blank()

    pl.semaphore_wait(barrier, sum(exists(move, 1).astype(jnp.int32) for move in moves))

    for message in x_in:
        message.start()
    for load in loads:
        load.wait()

    for s in range(2):
        row = cj - 1 if s == 0 else 0
        ys[s] = fields[:, :, row, :]
        for t in range(2):
            plane = ci - 1 if t == 0 else 0
            xys[t * 2 + s] = jnp.concatenate(
                [fields[:, plane, row, :], jnp.zeros((2, ck), F32)], axis=0
            )
    for message in y_in:
        message.start()

    xa, xb, lx = pair_weights(pos[0:1])
    ya, yb, ly = pair_weights(pos[1:2])
    za, zb, lz = pair_weights(pos[2:3])
    i0 = li[...] + lx
    j0 = lj[...] + ly
    k0 = lk[...] + lz
    codes = []
    for a, wa in enumerate((xa, xb)):
        for b, wb in enumerate((ya, yb)):
            i, j = i0 + a, j0 + b
            out_i = (i < 0) | (i >= ci)
            out_j = (j < 0) | (j >= cj)
            si = jnp.where(i < 0, 0, 1)
            sj = jnp.where(j < 0, 0, 1)
            code = jnp.where(
                out_i,
                jnp.where(out_j, inner + xy_row + si * 2 + sj, inner + si * cj + j),
                jnp.where(out_j, inner + y_row + sj * ci + i, i * cj + j),
            )
            codes.append((code, wa * wb))
    block = 128
    for start in range(0, planes, block):
        rows = lax.broadcasted_iota(jnp.int32, (block, slots), 0) + start
        table = jnp.zeros((block, slots), F32)
        for code, weight in codes:
            table = jnp.where(rows == code, weight, table)
        high, low = split(table)
        w_hi[start : start + block] = high
        w_lo[start : start + block] = low
    lines = lax.broadcasted_iota(jnp.int32, (ck, slots), 0)
    line[...] = jnp.where(lines == k0, za, jnp.where(lines == k0 + 1, zb, 0.0))
    rim = (jnp.where(k0 < 0, za, 0.0), jnp.where(k0 + 1 >= ck, zb, 0.0))

    zs[...] = jnp.zeros_like(zs)

    def lay(f, first, flat):
        wide = flat.shape[0]
        turned = flat.T
        high, low = split(turned)
        ft_hi[f * ck : (f + 1) * ck, first : first + wide] = high
        ft_lo[f * ck : (f + 1) * ck, first : first + wide] = low
        zs[0, f : f + 1, first : first + wide] = turned[ck - 1 : ck]
        zs[1, f : f + 1, first : first + wide] = turned[0:1]

    for f in range(6):
        lay(f, 0, fields[f].reshape(inner, ck))

    width = 256

    def sample(first, last, fresh):
        for s in range(0, slots, width):
            here = slice(s, s + width)
            got = nn(ft_hi[:, first:last], w_hi[first:last, here])
            got += nn(ft_hi[:, first:last], w_lo[first:last, here])
            got += nn(ft_lo[:, first:last], w_hi[first:last, here])
            for f in range(6):
                part = jnp.sum(
                    got[f * ck : (f + 1) * ck] * line[:, here], axis=0, keepdims=True
                )
                if fresh:
                    sampled[f : f + 1, here] = part
                else:
                    sampled[f : f + 1, here] += part

    sample(0, inner, True)

    for message in x_in + y_in:
        message.arrive()
    for f in range(6):
        flat = jnp.concatenate(
            [xh[0, f], xh[1, f], yh[0, f], yh[1, f]]
            + [xyh[q, f : f + 1] for q in range(4)]
            + [jnp.zeros((outer - xy_row - 4, ck), F32)],
            axis=0,
        )
        lay(f, inner, flat)
    for message in z_in:
        message.start()
    sample(inner, planes, False)
    for message in z_in:
        message.arrive()
    ends = jnp.concatenate([zh[0], zh[1]], axis=0)
    end_hi, end_lo = split(ends)
    got = nn(end_hi, w_hi[...]) + nn(end_hi, w_lo[...]) + nn(end_lo, w_hi[...])
    gas = sampled[...] + got[0:8] * rim[0] + got[8:16] * rim[1]

    live = lax.broadcasted_iota(jnp.int32, (1, slots), 1) // TILE < tally[0]
    q = size[...]
    tp = heat[...]
    v = mot[...]
    drag = step_time / (0.5 * q)
    v_new = (v + drag * gas[0:3]) / (1.0 + drag)
    mass = q * jnp.sqrt(q)
    share = jnp.exp(4.0 * (tp - 1.0))
    decay = step_time * evap_rate * gas[5:6] * (share - gas[4:5])
    q_new = q - decay
    mass_new = q_new * jnp.sqrt(q_new)
    conduct = step_time * heat_rate * gas[5:6] / q
    tp_new = (tp + conduct * gas[3:4]) / (1.0 + conduct) - boiling_energy_drain * decay / q
    state[0:3] = jnp.where(live, v_new, v)
    state[3:4] = jnp.where(live, tp_new, tp)
    state[4:5] = jnp.where(live, q_new, q)
    push = jnp.where(live, mass * (v - v_new), 0.0)
    terms = [
        push[0:1],
        push[1:2],
        push[2:3],
        jnp.where(live, mass * (tp - tp_new), 0.0),
        jnp.where(live, mass - mass_new, 0.0),
    ]
    stack = jnp.concatenate(terms + [jnp.zeros((3, slots), F32)], axis=0)
    ends = jnp.concatenate([stack * rim[1], stack * rim[0]], axis=0)
    end_hi, end_lo = split(ends)
    got = nt(end_hi, w_hi[...]) + nt(end_hi, w_lo[...]) + nt(end_lo, w_hi[...])
    dzs[0] = got[0:8]
    dzs[1] = got[8:16]
    for message in z_out:
        message.start()

    for c in range(5):
        high, low = split(line[...] * terms[c])
        src_hi[c * ck : (c + 1) * ck] = high
        src_lo[c * ck : (c + 1) * ck] = low

    def spread(first, last, low, high):
        got = nt(w_hi[first:last], src_hi[low:high])
        got += nt(w_hi[first:last], src_lo[low:high])
        got += nt(w_lo[first:last], src_hi[low:high])
        return got

    pick_row = lax.broadcasted_iota(jnp.int32, (32, 5 * ck), 0)
    pick_col = lax.broadcasted_iota(jnp.int32, (32, 5 * ck), 1)
    pick_row = jnp.where(pick_row >= 16, pick_row - 16, pick_row)
    target = jnp.where(pick_row >= 8, (pick_row - 8) * ck + ck - 1, pick_row * ck)
    pick = jnp.where(target == pick_col, 1.0, 0.0).astype(BF16)

    spans = [(c, min(c + 2, 5)) for c in range(0, 5, 2)]
    halo = [spread(inner, planes, a * ck, b * ck) for a, b in spans]
    for message in z_out:
        message.arrive()
    ends = jnp.concatenate([dzr[0], dzr[1]], axis=0)
    end_hi, end_lo = split(ends)
    ends = jnp.concatenate([end_hi, end_lo], axis=0)
    for part, (a, b) in zip(halo, spans):
        part = part + tn(ends[:, inner:], pick[:, a * ck : b * ck])
        for c in range(a, b):
            piece = part[:, (c - a) * ck : (c - a + 1) * ck]
            dxs[1, c] = piece[0:cj]
            dxs[0, c] = piece[cj : 2 * cj]
            dys[1, c] = piece[y_row : y_row + ci]
            dys[0, c] = piece[y_row + ci : y_row + 2 * ci]
            for n in range(4):
                dxys[3 - n, c : c + 1] = piece[xy_row + n : xy_row + n + 1]
    for message in x_out + xy_out:
        message.start()

    for a, b in spans:
        part = spread(0, inner, a * ck, b * ck) + tn(ends[:, :inner], pick[:, a * ck : b * ck])
        for c in range(a, b):
            dep[c] = part[:, (c - a) * ck : (c - a + 1) * ck].reshape(ci, cj, ck)

    for message in x_out + xy_out:
        message.arrive()
    for s in range(2):
        plane = 0 if s == 0 else ci - 1
        dep[:, plane] += dxr[s]
    for s in range(2):
        row = 0 if s == 0 else cj - 1
        dep[:, :, row, :] += dyr[s]
        for t in range(2):
            plane = 0 if t == 0 else ci - 1
            dep[:, plane, row, :] += dxyr[t * 2 + s, 0:5]
    for message in x_in + y_in + z_in + z_out + x_out + xy_out:
        message.leave()


def local(counts, vel, sca, pos, mot, heat, size, li, lj, lk, tally):
    ci, cj, ck = vel.shape[1:]
    slots = heat.shape[0]
    outer = 2 * cj + 2 * ci + 4
    planes = ci * cj + -(-outer // 128) * 128
    vmem = pl.BlockSpec(memory_space=pltpu.VMEM)
    row = lambda value: value.reshape(1, slots)
    messages = 24
    scratch = [
        pltpu.VMEM((6, ci, cj, ck), F32),
        pltpu.VMEM((6 * ck, planes), BF16),
        pltpu.VMEM((6 * ck, planes), BF16),
        pltpu.VMEM((planes, slots), BF16),
        pltpu.VMEM((planes, slots), BF16),
        pltpu.VMEM((ck, slots), F32),
        pltpu.VMEM((5 * ck, slots), BF16),
        pltpu.VMEM((5 * ck, slots), BF16),
        pltpu.VMEM((8, slots), F32),
        pltpu.VMEM((2, 6, cj, ck), F32),
        pltpu.VMEM((2, 6, ci, ck), F32),
        pltpu.VMEM((4, 8, ck), F32),
        pltpu.VMEM((2, 8, planes), F32),
        pltpu.VMEM((2, 6, ci, ck), F32),
        pltpu.VMEM((4, 8, ck), F32),
        pltpu.VMEM((2, 8, planes), F32),
        pltpu.VMEM((2, 5, cj, ck), F32),
        pltpu.VMEM((2, 5, ci, ck), F32),
        pltpu.VMEM((4, 8, ck), F32),
        pltpu.VMEM((2, 8, planes), F32),
        pltpu.VMEM((2, 5, cj, ck), F32),
        pltpu.VMEM((2, 5, ci, ck), F32),
        pltpu.VMEM((4, 8, ck), F32),
        pltpu.VMEM((2, 8, planes), F32),
        pltpu.SemaphoreType.DMA((2,)),
        pltpu.SemaphoreType.DMA((messages,)),
        pltpu.SemaphoreType.DMA((messages,)),
    ]
    return pl.pallas_call(
        functools.partial(kernel, counts),
        out_shape=(
            jax.ShapeDtypeStruct((5, ci, cj, ck), F32),
            jax.ShapeDtypeStruct((5, slots), F32),
        ),
        in_specs=[pl.BlockSpec(memory_space=pl.ANY)] * 2
        + [vmem] * 7
        + [pl.BlockSpec(memory_space=pltpu.SMEM)],
        out_specs=(vmem, vmem),
        scratch_shapes=scratch,
        compiler_params=pltpu.CompilerParams(collective_id=0, has_side_effects=True),
    )(vel, sca, pos, mot, row(heat), row(size), row(li), row(lj), row(lk), tally)


def solution(mesh):
    bricks = P(None, AXES[0], AXES[1], AXES[2])
    rows = P(None, AXES)
    flat = P(AXES)
    counts = tuple(mesh.shape[axis] for axis in AXES)
    return jax.shard_map(
        functools.partial(local, counts),
        mesh=mesh,
        in_specs=(bricks, bricks, rows, rows) + (flat,) * 6,
        out_specs=(bricks, rows),
        check_vma=False,
    )
```

```python
import functools

import jax
import jax.numpy as jnp
from jax import lax
from jax.experimental import pallas as pl
from jax.experimental.pallas import tpu as pltpu
from jax.sharding import PartitionSpec as P

TILE = 128
AXES = ("gx", "gy", "gz")
MESH = pl.DeviceIdType.MESH
F32 = jnp.float32
BF16 = jnp.bfloat16

step_time = 0.25
evap_rate = 1.0
heat_rate = 2.0
boiling_energy_drain = 0.3

X_MOVES = ((1, 0, 0, 0), (-1, 0, 0, 1))
Y_MOVES = ((0, 1, 0, 0), (0, -1, 0, 1))
XY_MOVES = ((1, 1, 0, 0), (1, -1, 0, 1), (-1, 1, 0, 2), (-1, -1, 0, 3))
Z_MOVES = ((0, 0, 1, 0), (0, 0, -1, 1))


def split(value):
    high = value.astype(BF16)
    return high, (value - high.astype(F32)).astype(BF16)


def nn(a, b):
    return lax.dot_general(a, b, (((1,), (0,)), ((), ())), preferred_element_type=F32)


def nt(a, b):
    return lax.dot_general(a, b, (((1,), (1,)), ((), ())), preferred_element_type=F32)


def tn(a, b):
    return lax.dot_general(a, b, (((0,), (0,)), ((), ())), preferred_element_type=F32)


def pair_weights(offset):
    lower = jnp.where(offset < 0.0, -1.0, 0.0)
    first = jnp.maximum(0.0, 1.0 - jnp.abs(offset - lower))
    second = jnp.maximum(0.0, 1.0 - jnp.abs(offset - (lower + 1.0)))
    return first, second, jnp.where(offset < 0.0, -1, 0)


def kernel(
    counts,
    vel,
    sca,
    pos_in,
    mot_in,
    heat_in,
    size_in,
    li_in,
    lj_in,
    lk_in,
    tally,
    dep,
    state,
    pos,
    mot,
    heat,
    size,
    li,
    lj,
    lk,
    fields,
    ft,
    w_hi,
    w_lo,
    line,
    src_hi,
    src_lo,
    sampled,
    xh,
    yh,
    xyh,
    zh,
    ys,
    xys,
    zs,
    dxs,
    dys,
    dxys,
    dzs,
    dxr,
    dyr,
    dxyr,
    dzr,
    load_sem,
    send_sem,
    recv_sem,
):
    ci, cj, ck = vel.shape[1:]
    slots = heat_in.shape[1]
    inner = ci * cj
    planes = w_hi.shape[0]
    outer = planes - inner
    y_row = 2 * cj
    xy_row = y_row + 2 * ci
    me = [lax.axis_index(axis) for axis in AXES]

    def exists(move, sign):
        good = None
        for d in range(3):
            step = sign * move[d]
            if step == 1:
                test = me[d] < counts[d] - 1
            elif step == -1:
                test = me[d] > 0
            else:
                continue
            good = test if good is None else jnp.logical_and(good, test)
        return good

    def peer(move):
        return tuple(lax.rem(me[d] + move[d] + counts[d], counts[d]) for d in range(3))

    moves = X_MOVES + Y_MOVES + XY_MOVES + Z_MOVES

    class Message:
        def __init__(self, number, move, src, dst):
            self.move = move
            self.dst = dst
            self.copy = pltpu.make_async_remote_copy(
                src_ref=src,
                dst_ref=dst,
                send_sem=send_sem.at[number],
                recv_sem=recv_sem.at[number],
                device_id=peer(move),
                device_id_type=MESH,
            )

        def start(self):
            @pl.when(exists(self.move, 1))
            def _():
                self.copy.start()

        def blank(self):
            @pl.when(jnp.logical_not(exists(self.move, -1)))
            def _():
                self.dst[...] = jnp.zeros(self.dst.shape, F32)

        def arrive(self):
            @pl.when(exists(self.move, -1))
            def _():
                self.copy.wait_recv()

        def leave(self):
            @pl.when(exists(self.move, 1))
            def _():
                self.copy.wait_send()

    x_in, y_in, z_in, x_out, xy_out, z_out = [], [], [], [], [], []
    number = 0

    def add(group, move, src, dst):
        nonlocal number
        group.append(Message(number, move, src, dst))
        number += 1

    for move in X_MOVES:
        row = ci - 1 if move[0] > 0 else 0
        add(x_in, move, vel.at[:, row], xh.at[move[3], 0:3])
        add(x_in, move, sca.at[:, row], xh.at[move[3], 3:6])
    for move in Y_MOVES:
        add(y_in, move, ys.at[move[3]], yh.at[move[3]])
    for move in XY_MOVES:
        add(y_in, move, xys.at[move[3]], xyh.at[move[3]])
    for move in Z_MOVES:
        add(z_in, move, zs.at[move[3]], zh.at[move[3]])
    for move in Z_MOVES:
        add(z_out, move, dzs.at[move[3]], dzr.at[move[3]])
    for move in X_MOVES:
        add(x_out, move, dxs.at[move[3]], dxr.at[move[3]])
    for move in Y_MOVES:
        add(xy_out, move, dys.at[move[3]], dyr.at[move[3]])
    for move in XY_MOVES:
        add(xy_out, move, dxys.at[move[3]], dxyr.at[move[3]])

    barrier = pltpu.get_barrier_semaphore()
    for move in moves:

        @pl.when(exists(move, 1))
        def _():
            pl.semaphore_signal(barrier, inc=1, device_id=peer(move), device_id_type=MESH)

    loads = [
        pltpu.make_async_copy(vel, fields.at[0:3], load_sem.at[0]),
        pltpu.make_async_copy(sca, fields.at[3:6], load_sem.at[1]),
    ]
    pairs = ((pos_in, pos), (li_in, li), (lj_in, lj), (lk_in, lk))
    pairs += ((mot_in, mot), (heat_in, heat), (size_in, size))
    smalls = [
        pltpu.make_async_copy(a, b, load_sem.at[2 + n]) for n, (a, b) in enumerate(pairs)
    ]
    for load in smalls + loads:
        load.start()
    for message in x_in + y_in + z_in + z_out + x_out + xy_out:
        message.blank()

    for load in smalls:
        load.wait()

    xa, xb, lx = pair_weights(pos[0:1])
    ya, yb, ly = pair_weights(pos[1:2])
    za, zb, lz = pair_weights(pos[2:3])
    i0 = li[...] + lx
    j0 = lj[...] + ly
    k0 = lk[...] + lz
    codes = []
    for a, wa in enumerate((xa, xb)):
        for b, wb in enumerate((ya, yb)):
            i, j = i0 + a, j0 + b
            out_i = (i < 0) | (i >= ci)
            out_j = (j < 0) | (j >= cj)
            si = jnp.where(i < 0, 0, 1)
            sj = jnp.where(j < 0, 0, 1)
            code = jnp.where(
                out_i,
                jnp.where(out_j, inner + xy_row + si * 2 + sj, inner + si * cj + j),
                jnp.where(out_j, inner + y_row + sj * ci + i, i * cj + j),
            )
            codes.append((code, wa * wb))
    block = 128
    for start in range(0, planes, block):
        rows = lax.broadcasted_iota(jnp.int32, (block, slots), 0) + start
        table = jnp.zeros((block, slots), F32)
        for code, weight in codes:
            table = jnp.where(rows == code, weight, table)
        high, low = split(table)
        w_hi[start : start + block] = high
        w_lo[start : start + block] = low
    lines = lax.broadcasted_iota(jnp.int32, (ck, slots), 0)
    line[...] = jnp.where(lines == k0, za, jnp.where(lines == k0 + 1, zb, 0.0))
    rim = (jnp.where(k0 < 0, za, 0.0), jnp.where(k0 + 1 >= ck, zb, 0.0))

    pl.semaphore_wait(barrier, sum(exists(move, 1).astype(jnp.int32) for move in moves))

    for message in x_in:
        message.start()
    for load in loads:
        load.wait()

    for s in range(2):
        row = cj - 1 if s == 0 else 0
        ys[s] = fields[:, :, row, :]
        for t in range(2):
            plane = ci - 1 if t == 0 else 0
            xys[t * 2 + s] = jnp.concatenate(
                [fields[:, plane, row, :], jnp.zeros((2, ck), F32)], axis=0
            )
    for message in y_in:
        message.start()

    zs[...] = jnp.zeros_like(zs)

    def lay(f, first, flat):
        wide = flat.shape[0]
        turned = flat.T
        high, low = split(turned)
        ft[f * ck : (f + 1) * ck, first : first + wide] = high
        ft[(6 + f) * ck : (7 + f) * ck, first : first + wide] = low
        zs[0, f : f + 1, first : first + wide] = turned[ck - 1 : ck]
        zs[1, f : f + 1, first : first + wide] = turned[0:1]

    for f in range(6):
        lay(f, 0, fields[f].reshape(inner, ck))

    width = 256

    def sample(first, last, fresh):
        for s in range(0, slots, width):
            here = slice(s, s + width)
            both = nn(ft[:, first:last], w_hi[first:last, here])
            got = both[: 6 * ck] + both[6 * ck :]
            got += nn(ft[: 6 * ck, first:last], w_lo[first:last, here])
            for f in range(6):
                part = jnp.sum(
                    got[f * ck : (f + 1) * ck] * line[:, here], axis=0, keepdims=True
                )
                if fresh:
                    sampled[f : f + 1, here] = part
                else:
                    sampled[f : f + 1, here] += part

    sample(0, inner, True)

    for message in x_in + y_in:
        message.arrive()
    for f in range(6):
        flat = jnp.concatenate(
            [xh[0, f], xh[1, f], yh[0, f], yh[1, f]]
            + [xyh[q, f : f + 1] for q in range(4)]
            + [jnp.zeros((outer - xy_row - 4, ck), F32)],
            axis=0,
        )
        lay(f, inner, flat)
    for message in z_in:
        message.start()
    sample(inner, planes, False)
    for message in z_in:
        message.arrive()
    ends = jnp.concatenate([zh[0], zh[1]], axis=0)
    end_hi, end_lo = split(ends)
    both = nn(jnp.concatenate([end_hi, end_lo], axis=0), w_hi[...])
    got = both[0:16] + both[16:32] + nn(end_hi, w_lo[...])
    gas = sampled[...] + got[0:8] * rim[0] + got[8:16] * rim[1]

    live = lax.broadcasted_iota(jnp.int32, (1, slots), 1) // TILE < tally[0]
    q = size[...]
    tp = heat[...]
    v = mot[...]
    drag = step_time / (0.5 * q)
    v_new = (v + drag * gas[0:3]) / (1.0 + drag)
    mass = q * jnp.sqrt(q)
    share = jnp.exp(4.0 * (tp - 1.0))
    decay = step_time * evap_rate * gas[5:6] * (share - gas[4:5])
    q_new = q - decay
    mass_new = q_new * jnp.sqrt(q_new)
    conduct = step_time * heat_rate * gas[5:6] / q
    tp_new = (tp + conduct * gas[3:4]) / (1.0 + conduct) - boiling_energy_drain * decay / q
    state[0:3] = jnp.where(live, v_new, v)
    state[3:4] = jnp.where(live, tp_new, tp)
    state[4:5] = jnp.where(live, q_new, q)
    push = jnp.where(live, mass * (v - v_new), 0.0)
    terms = [
        push[0:1],
        push[1:2],
        push[2:3],
        jnp.where(live, mass * (tp - tp_new), 0.0),
        jnp.where(live, mass - mass_new, 0.0),
    ]
    stack = jnp.concatenate(terms + [jnp.zeros((3, slots), F32)], axis=0)
    ends = jnp.concatenate([stack * rim[1], stack * rim[0]], axis=0)
    high, low = split(ends)
    src_hi[5 * ck : 5 * ck + 16] = high
    src_lo[5 * ck : 5 * ck + 16] = low
    for c in (4, 0, 1, 2, 3):
        high, low = split(line[...] * terms[c])
        src_hi[c * ck : (c + 1) * ck] = high
        src_lo[c * ck : (c + 1) * ck] = low

    def spread(first, last, low, high):
        got = nt(w_hi[first:last], src_hi[low:high])
        got += nt(w_hi[first:last], src_lo[low:high])
        got += nt(w_lo[first:last], src_hi[low:high])
        return got

    pick_row = lax.broadcasted_iota(jnp.int32, (32, 5 * ck), 0)
    pick_col = lax.broadcasted_iota(jnp.int32, (32, 5 * ck), 1)
    pick_row = jnp.where(pick_row >= 16, pick_row - 16, pick_row)
    target = jnp.where(pick_row >= 8, (pick_row - 8) * ck + ck - 1, pick_row * ck)
    pick = jnp.where(target == pick_col, 1.0, 0.0).astype(BF16)

    spans = ((0, 2), (2, 4), (4, 5))
    tail = spread(0, planes, 4 * ck, 5 * ck + 16)
    turned = tail[:, ck:].T
    dzs[0] = turned[0:8]
    dzs[1] = turned[8:16]
    for message in z_out:
        message.start()
    halo = [spread(inner, planes, a * ck, b * ck) for a, b in spans[:2]]
    halo.append(tail[inner:, :ck])
    for message in z_out:
        message.arrive()
    ends = jnp.concatenate([dzr[0], dzr[1]], axis=0)
    end_hi, end_lo = split(ends)
    ends = jnp.concatenate([end_hi, end_lo], axis=0)
    for part, (a, b) in zip(halo, spans):
        part = part + tn(ends[:, inner:], pick[:, a * ck : b * ck])
        for c in range(a, b):
            piece = part[:, (c - a) * ck : (c - a + 1) * ck]
            dxs[1, c] = piece[0:cj]
            dxs[0, c] = piece[cj : 2 * cj]
            dys[1, c] = piece[y_row : y_row + ci]
            dys[0, c] = piece[y_row + ci : y_row + 2 * ci]
            for n in range(4):
                dxys[3 - n, c : c + 1] = piece[xy_row + n : xy_row + n + 1]
    for message in x_out + xy_out:
        message.start()

    for a, b in spans[::-1]:
        part = tail[:inner, :ck] if a == 4 else spread(0, inner, a * ck, b * ck)
        part = part + tn(ends[:, :inner], pick[:, a * ck : b * ck])
        for c in range(a, b):
            dep[c] = part[:, (c - a) * ck : (c - a + 1) * ck].reshape(ci, cj, ck)

    for message in x_out + xy_out:
        message.arrive()
    for s in range(2):
        plane = 0 if s == 0 else ci - 1
        dep[:, plane] += dxr[s]
    for s in range(2):
        row = 0 if s == 0 else cj - 1
        dep[:, :, row, :] += dyr[s]
        for t in range(2):
            plane = 0 if t == 0 else ci - 1
            dep[:, plane, row, :] += dxyr[t * 2 + s, 0:5]
    for message in x_in + y_in + z_in + z_out + x_out + xy_out:
        message.leave()


def local(counts, vel, sca, pos, mot, heat, size, li, lj, lk, tally):
    ci, cj, ck = vel.shape[1:]
    slots = heat.shape[0]
    outer = 2 * cj + 2 * ci + 4
    planes = ci * cj + -(-outer // 128) * 128
    vmem = pl.BlockSpec(memory_space=pltpu.VMEM)
    row = lambda value: value.reshape(1, slots)
    messages = 24
    scratch = [pltpu.VMEM((3, slots), F32)] * 2 + [pltpu.VMEM((1, slots), F32)] * 2
    scratch += [pltpu.VMEM((1, slots), jnp.int32)] * 3
    scratch += [
        pltpu.VMEM((6, ci, cj, ck), F32),
        pltpu.VMEM((12 * ck, planes), BF16),
        pltpu.VMEM((planes, slots), BF16),
        pltpu.VMEM((planes, slots), BF16),
        pltpu.VMEM((ck, slots), F32),
        pltpu.VMEM((5 * ck + 16, slots), BF16),
        pltpu.VMEM((5 * ck + 16, slots), BF16),
        pltpu.VMEM((8, slots), F32),
        pltpu.VMEM((2, 6, cj, ck), F32),
        pltpu.VMEM((2, 6, ci, ck), F32),
        pltpu.VMEM((4, 8, ck), F32),
        pltpu.VMEM((2, 8, planes), F32),
        pltpu.VMEM((2, 6, ci, ck), F32),
        pltpu.VMEM((4, 8, ck), F32),
        pltpu.VMEM((2, 8, planes), F32),
        pltpu.VMEM((2, 5, cj, ck), F32),
        pltpu.VMEM((2, 5, ci, ck), F32),
        pltpu.VMEM((4, 8, ck), F32),
        pltpu.VMEM((2, 8, planes), F32),
        pltpu.VMEM((2, 5, cj, ck), F32),
        pltpu.VMEM((2, 5, ci, ck), F32),
        pltpu.VMEM((4, 8, ck), F32),
        pltpu.VMEM((2, 8, planes), F32),
        pltpu.SemaphoreType.DMA((9,)),
        pltpu.SemaphoreType.DMA((messages,)),
        pltpu.SemaphoreType.DMA((messages,)),
    ]
    return pl.pallas_call(
        functools.partial(kernel, counts),
        out_shape=(
            jax.ShapeDtypeStruct((5, ci, cj, ck), F32),
            jax.ShapeDtypeStruct((5, slots), F32),
        ),
        in_specs=[pl.BlockSpec(memory_space=pltpu.HBM)] * 9
        + [pl.BlockSpec(memory_space=pltpu.SMEM)],
        out_specs=(vmem, vmem),
        scratch_shapes=scratch,
        compiler_params=pltpu.CompilerParams(collective_id=0, has_side_effects=True),
    )(vel, sca, pos, mot, row(heat), row(size), row(li), row(lj), row(lk), tally)


def solution(mesh):
    bricks = P(None, AXES[0], AXES[1], AXES[2])
    rows = P(None, AXES)
    flat = P(AXES)
    counts = tuple(mesh.shape[axis] for axis in AXES)
    return jax.shard_map(
        functools.partial(local, counts),
        mesh=mesh,
        in_specs=(bricks, bricks, rows, rows) + (flat,) * 6,
        out_specs=(bricks, rows),
        check_vma=False,
    )
```
